32 devices in a mesh: head: 4 (over x, core), outer: 2 (over y), inner: 4 (over z).
Axes of the slice: x: 2, y: 2, z: 4, core: 2. Of those that a mesh axis runs over, the one named last changes fastest.
Arguments:
- queries: bfloat16 [8, 256, 4096], P(('outer', 'inner'), 'head'), may hold values from -120 to 120
- keys: bfloat16 [8, 256, 1024], P(('outer', 'inner'), 'head'), may hold values from -6 to 6
- values: bfloat16 [8, 256, 1024], P(('outer', 'inner'), 'head'), may hold values from -6 to 6
- doc_lengths: int32 [4], replicated, may hold values from 1 to 1024, 2048 in all
Outputs:
- attended: bfloat16 [8, 256, 4096], P(('outer', 'inner'), 'head')
The draws below stay inside these ranges and needn't reach their ends.
Inputs may be any that keep to these rules, and one draw needn't show every extreme that they name: `doc_lengths`: the documents of the packed sequence in order, summing to 2048.
All inputs are finite; a program needn't handle non-finite values.
Results may differ from the reference program's by a relative error of at most 0.0044.
Values may be sent and summed in bfloat16 or wider, within the bound.
A program may use at most 64 MiB of HBM per device.

```python
import math
import jax
import jax.numpy as jnp
import numpy as np
from jax import lax

HD = 128
QH = 32
KVH = 8
GROUP = 4
ROWS = 256
CTX = 8
REACH = 4
TOKENS = 2048
DOC_MOST = 1024
NDOCS = 4


def drawn_pair(key):
    base = jax.random.fold_in(key, 4242)
    keys_raw = jax.random.truncated_normal(jax.random.fold_in(base, 1), -6.0, 6.0, (CTX, ROWS, KVH, HD), jnp.float32)
    query_raw = jax.random.truncated_normal(jax.random.fold_in(base, 2), -6.0, 6.0, (CTX, ROWS, KVH, GROUP, HD), jnp.float32)
    return (query_raw, keys_raw)


def draw_queries(key, part):
    query_raw, keys_raw = drawn_pair(key)
    return query_raw.reshape(CTX, ROWS, QH * HD).astype(jnp.bfloat16)


def draw_keys(key, part):
    query_raw, keys_raw = drawn_pair(key)
    return keys_raw.reshape(CTX, ROWS, KVH * HD).astype(jnp.bfloat16)


def steps_of(rng, dims, pieces, low, top_value):
    def one(position, parts):
        steps = jax.random.uniform(jax.random.fold_in(jax.random.fold_in(rng, 6), position), (parts,), jnp.float32, low / len(pieces), top_value / len(pieces))
        return jnp.repeat(jnp.exp(steps), dims[position] // parts).reshape((-1,) + (1,) * (len(dims) - position - 1))

    loudness = one(*pieces[0])
    for cut in pieces[1:]:
        loudness = loudness * one(*cut)
    return loudness


def profile(number_of, total, limit, lean):
    loads = [(1 << 20) // math.isqrt(rank ** lean) + 1 for rank in range(2, number_of + 1)]
    rest, holding = total - limit - (number_of - 1), [1] * (number_of - 1)
    while rest > 0:
        candidates = [i for i in range(number_of - 1) if holding[i] < limit]
        whole, left = sum([loads[i] for i in candidates]), rest
        for i in candidates:
            more = min(limit - holding[i], max(1, left * loads[i] // whole), rest)
            holding[i] = holding[i] + more
            rest = rest - more
    return np.array([limit] + holding)


def ragged(stream_key, amount, total, most, slope):
    if amount == 2:
        one = jax.random.randint(stream_key, (), max(1, total - most), min(most, total - 1) + 1)
        return jnp.stack([one, total - one])
    sizes = jnp.asarray(profile(amount, total, most, slope), jnp.int32)
    twos = (amount - 1) // 2
    source_of, taker = sizes[1:1 + 2 * twos:2], sizes[2:2 + 2 * twos:2]
    slack = jnp.minimum(source_of - 1, most - taker)
    moved = jax.random.randint(jax.random.fold_in(stream_key, 1), (twos,), 0, 1 << 20) % (slack + 1)
    sizes = sizes.at[1:1 + 2 * twos:2].set(source_of - moved).at[2:2 + 2 * twos:2].set(taker + moved)
    return sizes[jax.random.permutation(jax.random.fold_in(stream_key, 2), amount)]


def scatter_about(stream_key, shape, spread, limit, pieces=(), held_as=jnp.bfloat16):
    values = jax.random.normal(stream_key, shape, jnp.float32) * spread
    if len(pieces) > 0:
        values = steps_of(stream_key, shape, pieces, -0.22, 0.18) * values
    return jnp.clip(values, min=-limit, max=limit).astype(held_as)


def setup_inputs(seed: int = 0) -> dict:
    seeds = jax.random.split(jax.random.key(seed), 5)
    queries = draw_queries(jax.random.fold_in(seeds[4], 71), 0)
    keys = draw_keys(jax.random.fold_in(seeds[4], 71), 0)
    values = scatter_about(seeds[2], (CTX, ROWS, KVH * HD), 1.0, 6.0, ((0, 8), (1, 4)))
    doc_lengths = ragged(seeds[3], NDOCS, TOKENS, DOC_MOST, 1).astype(jnp.int32)
    return dict(queries=queries, keys=keys, values=values, doc_lengths=doc_lengths)


def doc_index(positions, doc_lengths):
    ends = jnp.cumsum(doc_lengths)
    return lax.optimization_barrier(jnp.sum((positions[:, None] >= ends[None, :]).astype(jnp.int32), axis=1))

def reference(queries, keys, values, doc_lengths):
    ctx_count = queries.shape[0]
    rows = queries.shape[1]
    margin = REACH * rows
    q_all = queries.reshape(ctx_count * rows, KVH, GROUP, HD)
    k_all = jnp.concatenate([jnp.zeros((margin, KVH, HD), keys.dtype), keys.reshape(ctx_count * rows, KVH, HD)], axis=0)
    v_all = jnp.concatenate([jnp.zeros((margin, KVH, HD), values.dtype), values.reshape(ctx_count * rows, KVH, HD)], axis=0)
    scale = 1.0 / math.sqrt(HD)

    def one_block(rank):
        start = (rank * rows).astype(jnp.int32)
        q_block = lax.dynamic_slice_in_dim(q_all, start, rows, 0).astype(jnp.float32)
        k_block = lax.dynamic_slice_in_dim(k_all, start, margin + rows, 0).astype(jnp.float32)
        v_block = lax.dynamic_slice_in_dim(v_all, start, margin + rows, 0).astype(jnp.float32)
        q_pos = start + jnp.arange(rows, dtype=jnp.int32)
        k_pos = start - margin + jnp.arange(margin + rows, dtype=jnp.int32)
        q_doc = doc_index(q_pos, doc_lengths)
        k_doc = doc_index(k_pos, doc_lengths)
        visible = (k_pos[None, :] >= 0) & (k_pos[None, :] <= q_pos[:, None]) & (k_doc[None, :] == q_doc[:, None])
        scores = jnp.einsum('qgeh,kgh->geqk', q_block, k_block) * scale
        peak = lax.optimization_barrier(jnp.max(jnp.where(visible[None, None], scores, -1e+30), axis=-1))
        weights = jnp.where(visible[None, None], jnp.exp(scores - peak[..., None]), 0.0)
        total = lax.optimization_barrier(jnp.sum(weights, axis=-1))
        rounded = lax.optimization_barrier(weights.astype(jnp.bfloat16)).astype(jnp.float32)
        summed = jnp.einsum('geqk,kgh->qgeh', rounded, v_block)
        result = summed / jnp.transpose(total, (2, 0, 1))[..., None]
        return result.astype(jnp.bfloat16).reshape(rows, KVH * GROUP * HD)
    return lax.map(one_block, jnp.arange(ctx_count, dtype=jnp.int32))
```

```python
import functools
import math

import jax
import jax.numpy as jnp
from jax import lax
from jax.experimental import pallas as pl
from jax.experimental.pallas import tpu as pltpu
from jax.sharding import PartitionSpec as P

HD = 128
MAXDOC = 4096
HIDDEN = -1e30
MESH = pl.DeviceIdType.MESH


def kernel(plan, docs, q_ref, k_ref, v_ref, out, kv_in, q_in, kv, q_all, done, bias, start, peak, total, summed,
           load_sem, own_sem, kv_send, kv_recv, q_send, q_recv, win_send, win_recv, out_send, out_recv, out_own):
    heads, inner, ranks, reach, part, kv_heads, group = plan
    rows = heads * part
    width = group * HD
    me = lax.axis_index("head")
    rank = lax.axis_index("outer") * inner + lax.axis_index("inner")

    def at_rank(other):
        return {"outer": lax.div(other, inner), "inner": lax.rem(other, inner)}

    def peer(step):
        return lax.rem(me + step, heads)

    def kv_columns(owner, g):
        return pl.ds(pl.multiple_of((owner * kv_heads + g) * HD, HD), HD)

    def q_columns(owner, g):
        return pl.ds(pl.multiple_of((owner * kv_heads + g) * width, HD), width)

    def part_of(owner):
        return pl.ds(pl.multiple_of(owner * part, part), part)

    loads = [
        pltpu.make_async_copy(k_ref.at[0], kv_in.at[0], load_sem.at[0]),
        pltpu.make_async_copy(v_ref.at[0], kv_in.at[1], load_sem.at[1]),
        pltpu.make_async_copy(q_ref.at[0], q_in, load_sem.at[2]),
    ]
    for copy in loads:
        copy.start()
    own = []
    for g in range(kv_heads):
        own.append([
            pltpu.make_async_copy(k_ref.at[0, :, kv_columns(me, g)], kv.at[0, g, 0, part_of(me)], own_sem.at[g, 0]),
            pltpu.make_async_copy(v_ref.at[0, :, kv_columns(me, g)], kv.at[0, g, 1, part_of(me)], own_sem.at[g, 1]),
            pltpu.make_async_copy(q_ref.at[0, :, q_columns(me, g)], q_all.at[g, part_of(me)], own_sem.at[g, 2]),
        ])
        for copy in own[g]:
            copy.start()

    barrier = pltpu.get_barrier_semaphore()
    for step in range(1, heads):
        pl.semaphore_signal(barrier, inc=1, device_id={"head": peer(step)}, device_id_type=MESH)
    for d in range(1, reach + 1):
        @pl.when(rank + d < ranks)
        def _():
            pl.semaphore_signal(barrier, inc=1, device_id=at_rank(rank + d), device_id_type=MESH)

        @pl.when(rank >= d)
        def _():
            pl.semaphore_signal(barrier, inc=1, device_id=at_rank(rank - d), device_id_type=MESH)
    partners = heads - 1 + jnp.minimum(rank, reach) + jnp.minimum(ranks - 1 - rank, reach)
    pl.semaphore_wait(barrier, partners)

    def kv_copy(step, g, c):
        return pltpu.make_async_remote_copy(
            src_ref=kv_in.at[c, :, kv_columns(peer(step), g)],
            dst_ref=kv.at[0, g, c, part_of(me)],
            send_sem=kv_send.at[step, g, c],
            recv_sem=kv_recv.at[step, g, c],
            device_id={"head": peer(step)},
            device_id_type=MESH,
        )

    def q_copy(step, g):
        return pltpu.make_async_remote_copy(
            src_ref=q_in.at[:, q_columns(peer(step), g)],
            dst_ref=q_all.at[g, part_of(me)],
            send_sem=q_send.at[step, g],
            recv_sem=q_recv.at[step, g],
            device_id={"head": peer(step)},
            device_id_type=MESH,
        )

    def window_copy(d, g):
        return pltpu.make_async_remote_copy(
            src_ref=kv.at[0, g],
            dst_ref=kv.at[d, g],
            send_sem=win_send.at[d, g],
            recv_sem=win_recv.at[d, g],
            device_id=at_rank(lax.rem(rank + d, ranks)),
            device_id_type=MESH,
        )

    def out_copy(step, g):
        return pltpu.make_async_remote_copy(
            src_ref=done.at[g, part_of(peer(step))],
            dst_ref=out.at[0, :, q_columns(me, g)],
            send_sem=out_send.at[step, g],
            recv_sem=out_recv.at[step, g],
            device_id={"head": peer(step)},
            device_id_type=MESH,
        )

    loads[0].wait()
    loads[1].wait()
    for g in range(kv_heads):
        for step in range(1, heads):
            for c in range(2):
                kv_copy(step, g, c).start()
    loads[2].wait()
    for g in range(kv_heads):
        for step in range(1, heads):
            q_copy(step, g).start()

    pos = rank * rows + lax.broadcasted_iota(jnp.int32, (rows, rows), 0)
    first = jnp.zeros((rows, rows), jnp.int32)
    end = jnp.int32(0)
    for i in range(docs.shape[0]):
        end = end + docs[i]
        first = jnp.where(pos >= end, end, first)
    start[...] = first

    for g in range(kv_heads):
        own[g][0].wait()
        own[g][1].wait()
        for step in range(1, heads):
            for c in range(2):
                kv_copy(step, g, c).wait_recv()
        for d in range(reach, 0, -1):
            @pl.when(rank + d < ranks)
            def _():
                window_copy(d, g).start()

    power = math.log2(math.e) / math.sqrt(HD)

    def attend(g, d, opening):
        base = (rank - d) * rows
        spot = base + lax.broadcasted_iota(jnp.int32, (rows, rows), 1)
        visible = spot >= start[...]
        if opening:
            visible = visible & (spot <= rank * rows + lax.broadcasted_iota(jnp.int32, (rows, rows), 0))
        bias[...] = jnp.where(visible, 0.0, HIDDEN)
        keys = kv[d, g, 0]
        values = kv[d, g, 1]
        for e in range(group):
            query = q_all[g, :, e * HD:(e + 1) * HD]
            scores = lax.dot_general(query, keys, (((1,), (1,)), ((), ())), preferred_element_type=jnp.float32)
            scores = scores + bias[...]
            high = jnp.max(scores, axis=1, keepdims=True)
            if not opening:
                before = peak[e]
                high = jnp.maximum(high, before)
                factor = jnp.exp2((before - high) * power)
            weights = jnp.exp2((scores - high) * power)
            sums = jnp.sum(weights, axis=1, keepdims=True)
            added = jnp.dot(weights.astype(jnp.bfloat16), values, preferred_element_type=jnp.float32)
            peak[e] = high
            if opening:
                total[e] = sums
                summed[e] = added
            else:
                total[e] = total[e] * factor + sums
                summed[e] = summed[e] * factor + added

    for g in range(kv_heads):
        own[g][2].wait()
        for step in range(1, heads):
            q_copy(step, g).wait_recv()
        attend(g, 0, True)

        @pl.loop(1, reach + 1)
        def _(d):
            @pl.when(rank >= d)
            def _():
                window_copy(d, g).wait_recv()
                attend(g, d, False)

        for e in range(group):
            done[g, :, e * HD:(e + 1) * HD] = (summed[e] / total[e]).astype(jnp.bfloat16)
        for step in range(1, heads):
            out_copy(step, g).start()
        pltpu.make_async_copy(done.at[g, part_of(me)], out.at[0, :, q_columns(me, g)], out_own.at[g]).start()

    for g in range(kv_heads):
        for step in range(1, heads):
            for c in range(2):
                kv_copy(step, g, c).wait_send()
            q_copy(step, g).wait_send()
            out_copy(step, g).wait()
        pltpu.make_async_copy(done.at[g, part_of(me)], out.at[0, :, q_columns(me, g)], out_own.at[g]).wait()
        for d in range(1, reach + 1):
            @pl.when(rank + d < ranks)
            def _():
                window_copy(d, g).wait_send()


def solution(mesh):
    heads = mesh.shape["head"]
    inner = mesh.shape["inner"]
    ranks = mesh.shape["outer"] * inner

    def body(queries, keys, values, doc_lengths):
        part = queries.shape[1]
        rows = part * heads
        kv_heads = keys.shape[2] // HD // heads
        group = queries.shape[2] // keys.shape[2]
        reach = min(MAXDOC // rows, ranks // 2)
        plan = (heads, inner, ranks, reach, part, kv_heads, group)
        anywhere = pl.BlockSpec(memory_space=pl.ANY)
        dma = pltpu.SemaphoreType.DMA
        return pl.pallas_call(
            functools.partial(kernel, plan),
            out_shape=jax.ShapeDtypeStruct(queries.shape, jnp.bfloat16),
            in_specs=[pl.BlockSpec(memory_space=pltpu.SMEM), anywhere, anywhere, anywhere],
            out_specs=anywhere,
            scratch_shapes=[
                pltpu.VMEM((2, part, keys.shape[2]), jnp.bfloat16),
                pltpu.VMEM((part, queries.shape[2]), jnp.bfloat16),
                pltpu.VMEM((reach + 1, kv_heads, 2, rows, HD), jnp.bfloat16),
                pltpu.VMEM((kv_heads, rows, group * HD), jnp.bfloat16),
                pltpu.VMEM((kv_heads, rows, group * HD), jnp.bfloat16),
                pltpu.VMEM((rows, rows), jnp.float32),
                pltpu.VMEM((rows, rows), jnp.int32),
                pltpu.VMEM((group, rows, 1), jnp.float32),
                pltpu.VMEM((group, rows, 1), jnp.float32),
                pltpu.VMEM((group, rows, HD), jnp.float32),
                dma((3,)),
                dma((kv_heads, 3)),
                dma((heads, kv_heads, 2)),
                dma((heads, kv_heads, 2)),
                dma((heads, kv_heads)),
                dma((heads, kv_heads)),
                dma((reach + 1, kv_heads)),
                dma((reach + 1, kv_heads)),
                dma((heads, kv_heads)),
                dma((heads, kv_heads)),
                dma((kv_heads,)),
            ],
            compiler_params=pltpu.CompilerParams(
                collective_id=0, has_side_effects=True, vmem_limit_bytes=32 * 1024 * 1024
            ),
            name="attention",
        )(doc_lengths, queries, keys, values)

    split = P(("outer", "inner"), "head", None)
    return jax.shard_map(
        body, mesh=mesh, in_specs=(split, split, split, P()), out_specs=split, check_vma=False
    )
```

```python
import functools
import math

import jax
import jax.numpy as jnp
from jax import lax
from jax.experimental import pallas as pl
from jax.experimental.pallas import tpu as pltpu
from jax.sharding import PartitionSpec as P

HD = 128
MAXDOC = 4096
HIDDEN = -1e30
MESH = pl.DeviceIdType.MESH


def kernel(plan, docs, q_ref, k_ref, v_ref, out, kv_in, q_in, kv, q_all, done, bias, start, peak, total, summed,
           load_sem, own_sem, kv_send, kv_recv, q_send, q_recv, up_send, down_send, direct_send, win_recv, out_send, out_recv, out_own):
    heads, inner, ranks, reach, part, kv_heads, group = plan
    rows = heads * part
    width = group * HD
    me = lax.axis_index("head")
    rank = lax.axis_index("outer") * inner + lax.axis_index("inner")

    def at_rank(other):
        return {"outer": lax.div(other, inner), "inner": lax.rem(other, inner)}

    pack = heads // 2
    half, spot_in = lax.div(me, pack), lax.rem(me, pack)

    def peer(step):
        side = half if step < pack else 1 - half
        return side * pack + lax.rem(spot_in + step % pack, pack)

    def kv_columns(owner, g):
        return pl.ds(pl.multiple_of((owner * kv_heads + g) * HD, HD), HD)

    def q_columns(owner, g):
        return pl.ds(pl.multiple_of((owner * kv_heads + g) * width, HD), width)

    def in_half(owner):
        return pl.ds(pl.multiple_of(lax.rem(owner, pack) * part, part), part)

    def part_of(owner):
        return pl.ds(pl.multiple_of(owner * part, part), part)

    place = lax.axis_index("inner")
    direct = [d for d in (reach, reach - 1) if d >= 1]
    has_up, has_down = place < inner - 1, place > 0

    def straight(d, at):
        return at < (d if d == reach else 1)

    sends = [(rank + d < ranks) & straight(d, lax.rem(rank + d, inner)) for d in direct]
    links = [(has_up, rank + 1), (has_down, rank - 1)]
    for d, wanted in zip(direct, sends):
        links.append((wanted, rank + d))
        links.append(((rank >= d) & straight(d, place), rank - d))

    loads = [
        pltpu.make_async_copy(k_ref.at[0], kv_in.at[0], load_sem.at[0]),
        pltpu.make_async_copy(v_ref.at[0], kv_in.at[1], load_sem.at[1]),
        pltpu.make_async_copy(q_ref.at[0], q_in, load_sem.at[2]),
    ]
    for copy in loads:
        copy.start()
    own = []
    for g in range(kv_heads):
        own.append([
            pltpu.make_async_copy(k_ref.at[0, :, kv_columns(me, g)], kv.at[0, g, half, 0, in_half(me)], own_sem.at[g, 0]),
            pltpu.make_async_copy(v_ref.at[0, :, kv_columns(me, g)], kv.at[0, g, half, 1, in_half(me)], own_sem.at[g, 1]),
            pltpu.make_async_copy(q_ref.at[0, :, q_columns(me, g)], q_all.at[g, part_of(me)], own_sem.at[g, 2]),
        ])
        for copy in own[g]:
            copy.start()

    barrier = pltpu.get_barrier_semaphore()
    for step in range(1, heads):
        pl.semaphore_signal(barrier, inc=1, device_id={"head": peer(step)}, device_id_type=MESH)
    partners = heads - 1
    for wanted, other in links:
        @pl.when(wanted)
        def _():
            pl.semaphore_signal(barrier, inc=1, device_id=at_rank(other), device_id_type=MESH)

        partners = partners + wanted.astype(jnp.int32)
    pl.semaphore_wait(barrier, partners)

    def kv_copy(step, g, c):
        return pltpu.make_async_remote_copy(
            src_ref=kv_in.at[c, :, kv_columns(peer(step), g)],
            dst_ref=kv.at[0, g, half, c, in_half(me)],
            send_sem=kv_send.at[step, g, c],
            recv_sem=kv_recv.at[step, g, c],
            device_id={"head": peer(step)},
            device_id_type=MESH,
        )

    def kv_arrival(step, g, c):
        side = half if step < pack else 1 - half
        source = lax.rem(spot_in + pack - step % pack, pack)
        return pltpu.make_async_remote_copy(
            src_ref=kv_in.at[c, :, kv_columns(peer(step), g)],
            dst_ref=kv.at[0, g, side, c, in_half(source)],
            send_sem=kv_send.at[step, g, c],
            recv_sem=kv_recv.at[step, g, c],
            device_id={"head": peer(step)},
            device_id_type=MESH,
        )

    def q_copy(step, g):
        return pltpu.make_async_remote_copy(
            src_ref=q_in.at[:, q_columns(peer(step), g)],
            dst_ref=q_all.at[g, part_of(me)],
            send_sem=q_send.at[step, g],
            recv_sem=q_recv.at[step, g],
            device_id={"head": peer(step)},
            device_id_type=MESH,
        )

    def window_copy(src, dst, g, part_half, other, sem):
        return pltpu.make_async_remote_copy(
            src_ref=kv.at[src, g, part_half],
            dst_ref=kv.at[dst, g, part_half],
            send_sem=sem,
            recv_sem=win_recv.at[dst, g, part_half],
            device_id=at_rank(other),
            device_id_type=MESH,
        )

    def up_copy(d, g, part_half):
        return window_copy(d, d + 1, g, part_half, lax.rem(rank + 1, ranks), up_send.at[d, g, part_half])

    def down_copy(d, g, part_half):
        return window_copy(d, d - 1, g, part_half, lax.rem(rank + ranks - 1, ranks), down_send.at[d, g, part_half])

    def direct_copy(i, g, part_half):
        return window_copy(0, direct[i], g, part_half, lax.rem(rank + direct[i], ranks), direct_send.at[i, g, part_half])

    def goes_up(d):
        return has_up & (place >= d) & (d < reach)

    def goes_down(d):
        return has_down & (place < d) & (rank >= d) & (d >= 2) & ((d < reach) | (place > 1))

    def out_copy(step, g):
        return pltpu.make_async_remote_copy(
            src_ref=done.at[g, part_of(peer(step))],
            dst_ref=out.at[0, :, q_columns(me, g)],
            send_sem=out_send.at[step, g],
            recv_sem=out_recv.at[step, g],
            device_id={"head": peer(step)},
            device_id_type=MESH,
        )

    loads[0].wait()
    loads[1].wait()
    for g in range(kv_heads):
        for step in range(1, heads):
            for c in range(2):
                kv_copy(step, g, c).start()
    loads[2].wait()
    for g in range(kv_heads):
        for step in range(1, heads):
            q_copy(step, g).start()

    pos = rank * rows + lax.broadcasted_iota(jnp.int32, (1, rows), 1)
    first = jnp.zeros((1, rows), jnp.int32)
    end = jnp.int32(0)
    for i in range(docs.shape[0]):
        end = end + docs[i]
        first = jnp.where(pos >= end, end, first)
    start[...] = first

    for side in range(2):
        part_half = half if side == 0 else 1 - half
        for g in range(kv_heads):
            if side == 0:
                own[g][0].wait()
                own[g][1].wait()
            for step in range(max(1, side * pack), (side + 1) * pack):
                for c in range(2):
                    kv_arrival(step, g, c).wait_recv()

            @pl.when(has_up)
            def _():
                up_copy(0, g, part_half).start()

            for i in range(len(direct)):
                @pl.when(sends[i])
                def _():
                    direct_copy(i, g, part_half).start()

    power = math.log2(math.e) / math.sqrt(HD)

    def attend(g, d, opening):
        spot = (rank - d) * rows + lax.broadcasted_iota(jnp.int32, (rows, rows), 0)
        visible = spot >= start[...]
        if opening:
            visible = visible & (spot <= rank * rows + lax.broadcasted_iota(jnp.int32, (rows, rows), 1))
        bias[...] = jnp.where(visible, 0.0, HIDDEN)
        keys = jnp.concatenate([kv[d, g, 0, 0], kv[d, g, 1, 0]], axis=0)
        values = jnp.concatenate([kv[d, g, 0, 1].T, kv[d, g, 1, 1].T], axis=1)
        for n in range(group):
            e = g * group + n
            query = q_all[g, :, n * HD:(n + 1) * HD]
            scores = lax.dot_general(keys, query, (((1,), (1,)), ((), ())), preferred_element_type=jnp.float32)
            scores = scores + bias[...]
            high = jnp.max(scores, axis=0, keepdims=True)
            if not opening:
                before = peak[e]
                high = jnp.maximum(high, before)
                factor = jnp.exp2((before - high) * power)
            weights = jnp.exp2((scores - high) * power)
            sums = jnp.sum(weights, axis=0, keepdims=True)
            added = jnp.dot(values, weights.astype(jnp.bfloat16), preferred_element_type=jnp.float32)
            peak[e] = high
            if opening:
                total[e] = sums
                summed[e] = added
            else:
                total[e] = total[e] * factor + sums
                summed[e] = summed[e] * factor + added

    for g in range(kv_heads):
        own[g][2].wait()
        for step in range(1, heads):
            q_copy(step, g).wait_recv()
        attend(g, 0, True)

    near = jnp.minimum(place, reach)
    across = reach - near

    @pl.loop(1, reach + 1)
    def _(k):
        d = jnp.where(near == 0, reach + 1 - k, jnp.where(k == 1, 1, jnp.where(k <= 1 + across, reach + 2 - k, k - across)))
        here = rank >= d
        for g in range(kv_heads):
            @pl.when(here)
            def _():
                for side in range(2):
                    part_half = half if side == 0 else 1 - half
                    up_arrival = window_copy(
                        0, d, g, part_half, lax.rem(rank + 1, ranks), up_send.at[0, g, part_half]
                    )
                    up_arrival.wait_recv()

                    @pl.when(goes_up(d))
                    def _():
                        up_copy(d, g, part_half).start()

                    @pl.when(goes_down(d))
                    def _():
                        down_copy(d, g, part_half).start()

                attend(g, d, False)

            @pl.when(k == reach)
            def _():
                for n in range(group):
                    e = g * group + n
                    done[g, :, n * HD:(n + 1) * HD] = (summed[e] / total[e]).astype(jnp.bfloat16).T
                for step in range(heads - 1, 0, -1):
                    out_copy(step, g).start()
                pltpu.make_async_copy(done.at[g, part_of(me)], out.at[0, :, q_columns(me, g)], out_own.at[g]).start()

    for g in range(kv_heads):
        for step in range(1, heads):
            for c in range(2):
                kv_copy(step, g, c).wait_send()
            q_copy(step, g).wait_send()
            out_copy(step, g).wait()
        pltpu.make_async_copy(done.at[g, part_of(me)], out.at[0, :, q_columns(me, g)], out_own.at[g]).wait()

        for side in range(2):
            for i in range(len(direct)):
                @pl.when(sends[i])
                def _():
                    direct_copy(i, g, side).wait_send()

            @pl.loop(0, reach + 1)
            def _(d):
                @pl.when(goes_up(d))
                def _():
                    up_copy(d, g, side).wait_send()

                @pl.when(goes_down(d))
                def _():
                    down_copy(d, g, side).wait_send()


def solution(mesh):
    heads = mesh.shape["head"]
    inner = mesh.shape["inner"]
    ranks = mesh.shape["outer"] * inner

    def body(queries, keys, values, doc_lengths):
        part = queries.shape[1]
        rows = part * heads
        kv_heads = keys.shape[2] // HD // heads
        group = queries.shape[2] // keys.shape[2]
        reach = min(MAXDOC // rows, ranks // 2)
        plan = (heads, inner, ranks, reach, part, kv_heads, group)
        anywhere = pl.BlockSpec(memory_space=pl.ANY)
        dma = pltpu.SemaphoreType.DMA
        return pl.pallas_call(
            functools.partial(kernel, plan),
            out_shape=jax.ShapeDtypeStruct(queries.shape, jnp.bfloat16),
            in_specs=[pl.BlockSpec(memory_space=pltpu.SMEM), anywhere, anywhere, anywhere],
            out_specs=anywhere,
            scratch_shapes=[
                pltpu.VMEM((2, part, keys.shape[2]), jnp.bfloat16),
                pltpu.VMEM((part, queries.shape[2]), jnp.bfloat16),
                pltpu.VMEM((reach + 1, kv_heads, 2, 2, rows // 2, HD), jnp.bfloat16),
                pltpu.VMEM((kv_heads, rows, group * HD), jnp.bfloat16),
                pltpu.VMEM((kv_heads, rows, group * HD), jnp.bfloat16),
                pltpu.VMEM((rows, rows), jnp.float32),
                pltpu.VMEM((1, rows), jnp.int32),
                pltpu.VMEM((kv_heads * group, 1, rows), jnp.float32),
                pltpu.VMEM((kv_heads * group, 1, rows), jnp.float32),
                pltpu.VMEM((kv_heads * group, HD, rows), jnp.float32),
                dma((3,)),
                dma((kv_heads, 3)),
                dma((heads, kv_heads, 2)),
                dma((heads, kv_heads, 2)),
                dma((heads, kv_heads)),
                dma((heads, kv_heads)),
                dma((reach + 1, kv_heads, 2)),
                dma((reach + 1, kv_heads, 2)),
                dma((2, kv_heads, 2)),
                dma((reach + 1, kv_heads, 2)),
                dma((heads, kv_heads)),
                dma((heads, kv_heads)),
                dma((kv_heads,)),
            ],
            compiler_params=pltpu.CompilerParams(
                collective_id=0, has_side_effects=True, vmem_limit_bytes=60 * 1024 * 1024
            ),
            name="attention",
        )(doc_lengths, queries, keys, values)

    split = P(("outer", "inner"), "head", None)
    return jax.shard_map(
        body, mesh=mesh, in_specs=(split, split, split, P()), out_specs=split, check_vma=False
    )
```

```python
import functools
import math

import jax
import jax.numpy as jnp
from jax import lax
from jax.experimental import pallas as pl
from jax.experimental.pallas import tpu as pltpu
from jax.sharding import PartitionSpec as P

HD = 128
MAXDOC = 4096
HIDDEN = -1e30
MESH = pl.DeviceIdType.MESH


def kernel(plan, docs, q_ref, k_ref, v_ref, out, kv_in, q_in, kv, q_all, done, bias, held, start, peak, total, summed,
           load_sem, own_sem, kv_send, kv_recv, q_send, q_recv, up_send, down_send, direct_send, win_recv, out_send, out_recv, out_own):
    heads, inner, ranks, reach, part, kv_heads, group = plan
    rows = heads * part
    width = group * HD
    me = lax.axis_index("head")
    rank = lax.axis_index("outer") * inner + lax.axis_index("inner")

    def at_rank(other):
        return {"outer": lax.div(other, inner), "inner": lax.rem(other, inner)}

    pack = heads // 2
    half, spot_in = lax.div(me, pack), lax.rem(me, pack)

    def peer(step):
        side = half if step < pack else 1 - half
        return side * pack + lax.rem(spot_in + step % pack, pack)

    def kv_columns(owner, g):
        return pl.ds(pl.multiple_of((owner * kv_heads + g) * HD, HD), HD)

    def q_columns(owner, g):
        return pl.ds(pl.multiple_of((owner * kv_heads + g) * width, HD), width)

    def in_half(owner):
        return pl.ds(pl.multiple_of(lax.rem(owner, pack) * part, part), part)

    def part_of(owner):
        return pl.ds(pl.multiple_of(owner * part, part), part)

    place = lax.axis_index("inner")
    direct = [d for d in (reach, reach - 1) if d >= 1]
    has_up, has_down = place < inner - 1, place > 0

    def straight(d, at):
        return at < (d if d == reach else 1)

    sends = [(rank + d < ranks) & straight(d, lax.rem(rank + d, inner)) for d in direct]
    links = [(has_up, rank + 1), (has_down, rank - 1)]
    for d, wanted in zip(direct, sends):
        links.append((wanted, rank + d))
        links.append(((rank >= d) & straight(d, place), rank - d))

    loads = [
        pltpu.make_async_copy(k_ref.at[0], kv_in.at[0], load_sem.at[0]),
        pltpu.make_async_copy(v_ref.at[0], kv_in.at[1], load_sem.at[1]),
        pltpu.make_async_copy(q_ref.at[0], q_in, load_sem.at[2]),
    ]
    for copy in loads:
        copy.start()
    own = []
    for g in range(kv_heads):
        own.append([
            pltpu.make_async_copy(k_ref.at[0, :, kv_columns(me, g)], kv.at[0, g, half, 0, in_half(me)], own_sem.at[g, 0]),
            pltpu.make_async_copy(v_ref.at[0, :, kv_columns(me, g)], kv.at[0, g, half, 1, in_half(me)], own_sem.at[g, 1]),
            pltpu.make_async_copy(q_ref.at[0, :, q_columns(me, g)], q_all.at[g, part_of(me)], own_sem.at[g, 2]),
        ])
        for copy in own[g]:
            copy.start()

    barrier = pltpu.get_barrier_semaphore()
    for step in range(1, heads):
        pl.semaphore_signal(barrier, inc=1, device_id={"head": peer(step)}, device_id_type=MESH)
    partners = heads - 1
    for wanted, other in links:
        @pl.when(wanted)
        def _():
            pl.semaphore_signal(barrier, inc=1, device_id=at_rank(other), device_id_type=MESH)

        partners = partners + wanted.astype(jnp.int32)
    pl.semaphore_wait(barrier, partners)

    def kv_copy(step, g, c):
        return pltpu.make_async_remote_copy(
            src_ref=kv_in.at[c, :, kv_columns(peer(step), g)],
            dst_ref=kv.at[0, g, half, c, in_half(me)],
            send_sem=kv_send.at[step, g, c],
            recv_sem=kv_recv.at[step, g, c],
            device_id={"head": peer(step)},
            device_id_type=MESH,
        )

    def kv_arrival(step, g, c):
        side = half if step < pack else 1 - half
        source = lax.rem(spot_in + pack - step % pack, pack)
        return pltpu.make_async_remote_copy(
            src_ref=kv_in.at[c, :, kv_columns(peer(step), g)],
            dst_ref=kv.at[0, g, side, c, in_half(source)],
            send_sem=kv_send.at[step, g, c],
            recv_sem=kv_recv.at[step, g, c],
            device_id={"head": peer(step)},
            device_id_type=MESH,
        )

    def q_copy(step, g):
        return pltpu.make_async_remote_copy(
            src_ref=q_in.at[:, q_columns(peer(step), g)],
            dst_ref=q_all.at[g, part_of(me)],
            send_sem=q_send.at[step, g],
            recv_sem=q_recv.at[step, g],
            device_id={"head": peer(step)},
            device_id_type=MESH,
        )

    def window_copy(src, dst, g, part_half, other, sem):
        return pltpu.make_async_remote_copy(
            src_ref=kv.at[src, g, part_half],
            dst_ref=kv.at[dst, g, part_half],
            send_sem=sem,
            recv_sem=win_recv.at[dst, g, part_half],
            device_id=at_rank(other),
            device_id_type=MESH,
        )

    def up_copy(d, g, part_half):
        return window_copy(d, d + 1, g, part_half, lax.rem(rank + 1, ranks), up_send.at[d, g, part_half])

    def down_copy(d, g, part_half):
        return window_copy(d, d - 1, g, part_half, lax.rem(rank + ranks - 1, ranks), down_send.at[d, g, part_half])

    def direct_copy(i, g, part_half):
        return window_copy(0, direct[i], g, part_half, lax.rem(rank + direct[i], ranks), direct_send.at[i, g, part_half])

    def goes_up(d):
        return has_up & (place >= d) & (d < reach)

    def goes_down(d):
        return has_down & (place < d) & (rank >= d) & (d >= 2) & ((d < reach) | (place > 1))

    def out_copy(step, g):
        return pltpu.make_async_remote_copy(
            src_ref=done.at[g, part_of(peer(step))],
            dst_ref=out.at[0, :, q_columns(me, g)],
            send_sem=out_send.at[step, g],
            recv_sem=out_recv.at[step, g],
            device_id={"head": peer(step)},
            device_id_type=MESH,
        )

    loads[0].wait()
    loads[1].wait()
    for g in range(kv_heads):
        for step in range(1, heads):
            for c in range(2):
                kv_copy(step, g, c).start()
    loads[2].wait()
    for g in range(kv_heads):
        for step in range(1, heads):
            q_copy(step, g).start()

    pos = rank * rows + lax.broadcasted_iota(jnp.int32, (1, rows), 1)
    first = jnp.zeros((1, rows), jnp.int32)
    end = jnp.int32(0)
    for i in range(docs.shape[0]):
        end = end + docs[i]
        first = jnp.where(pos >= end, end, first)
    start[...] = first

    for side in range(2):
        part_half = half if side == 0 else 1 - half
        for g in range(kv_heads):
            if side == 0:
                own[g][0].wait()
                own[g][1].wait()
            for step in range(max(1, side * pack), (side + 1) * pack):
                for c in range(2):
                    kv_arrival(step, g, c).wait_recv()

            @pl.when(has_up)
            def _():
                up_copy(0, g, part_half).start()

            for i in range(len(direct)):
                @pl.when(sends[i])
                def _():
                    direct_copy(i, g, part_half).start()

    power = math.log2(math.e) / math.sqrt(HD)

    def attend(g, d, opening):
        spot = (rank - d) * rows + lax.broadcasted_iota(jnp.int32, (rows, rows), 0)
        visible = spot >= start[...]
        if opening:
            visible = visible & (spot <= rank * rows + lax.broadcasted_iota(jnp.int32, (rows, rows), 1))
        bias[...] = jnp.where(visible, 0.0, HIDDEN)
        keys = jnp.concatenate([kv[d, g, 0, 0], kv[d, g, 1, 0]], axis=0)
        values = jnp.concatenate([kv[d, g, 0, 1].T, kv[d, g, 1, 1].T], axis=1)
        kept = bias[...]

        def score(n):
            query = q_all[g, :, n * HD:(n + 1) * HD]
            return lax.dot_general(keys, query, (((1,), (1,)), ((), ())), preferred_element_type=jnp.float32) + kept

        highs = []
        for n in range(group):
            scores = score(n)
            held[n] = scores
            highs.append(jnp.max(scores, axis=0, keepdims=True))
        for n in range(group):
            e = g * group + n
            high = highs[n]
            if not opening:
                before = peak[e]
                high = jnp.maximum(high, before)
                factor = jnp.exp2((before - high) * power)
            weights = jnp.exp2((held[n] - high) * power)
            sums = jnp.sum(weights, axis=0, keepdims=True)
            added = jnp.dot(values, weights.astype(jnp.bfloat16), preferred_element_type=jnp.float32)
            peak[e] = high
            if opening:
                total[e] = sums
                summed[e] = added
            else:
                total[e] = total[e] * factor + sums
                summed[e] = summed[e] * factor + added

    near = jnp.minimum(place, reach)
    across = reach - near

    def slot_at(k):
        later = jnp.where(k == 1, 1, jnp.where(k <= 1 + across, reach + 2 - k, k - across))
        return jnp.where(near == 0, reach + 1 - k, later)

    def receive(k, g, wanted):
        d = slot_at(k)

        @pl.when(wanted & (rank >= d))
        def _():
            for side in range(2):
                part_half = half if side == 0 else 1 - half
                window_copy(0, d, g, part_half, lax.rem(rank + 1, ranks), up_send.at[0, g, part_half]).wait_recv()

                @pl.when(goes_up(d))
                def _():
                    up_copy(d, g, part_half).start()

                @pl.when(goes_down(d))
                def _():
                    down_copy(d, g, part_half).start()

    last = slot_at(reach)
    hurry = goes_up(last) | goes_down(last)

    for g in range(kv_heads):
        receive(1, g, True)
        receive(2, g, True)
    for g in range(kv_heads):
        own[g][2].wait()
        for step in range(1, heads):
            q_copy(step, g).wait_recv()
        attend(g, 0, True)

    @pl.loop(1, reach + 1)
    def _(k):
        d = slot_at(k)
        for g in range(kv_heads):
            receive(k + 1, g, (k >= 2) & (k < reach) & ((k + 1 < reach) | hurry))
            receive(k, g, (k == reach) & (k > 2) & jnp.logical_not(hurry))

            @pl.when(rank >= d)
            def _():
                attend(g, d, False)

            @pl.when(k == reach)
            def _():
                for n in range(group):
                    e = g * group + n
                    done[g, :, n * HD:(n + 1) * HD] = (summed[e] / total[e]).astype(jnp.bfloat16).T
                for step in range(heads - 1, 0, -1):
                    out_copy(step, g).start()
                pltpu.make_async_copy(done.at[g, part_of(me)], out.at[0, :, q_columns(me, g)], out_own.at[g]).start()

    for g in range(kv_heads):
        for step in range(1, heads):
            for c in range(2):
                kv_copy(step, g, c).wait_send()
            q_copy(step, g).wait_send()
            out_copy(step, g).wait()
        pltpu.make_async_copy(done.at[g, part_of(me)], out.at[0, :, q_columns(me, g)], out_own.at[g]).wait()

        for side in range(2):
            for i in range(len(direct)):
                @pl.when(sends[i])
                def _():
                    direct_copy(i, g, side).wait_send()

            @pl.loop(0, reach + 1)
            def _(d):
                @pl.when(goes_up(d))
                def _():
                    up_copy(d, g, side).wait_send()

                @pl.when(goes_down(d))
                def _():
                    down_copy(d, g, side).wait_send()


def solution(mesh):
    heads = mesh.shape["head"]
    inner = mesh.shape["inner"]
    ranks = mesh.shape["outer"] * inner

    def body(queries, keys, values, doc_lengths):
        part = queries.shape[1]
        rows = part * heads
        kv_heads = keys.shape[2] // HD // heads
        group = queries.shape[2] // keys.shape[2]
        reach = min(MAXDOC // rows, ranks // 2)
        plan = (heads, inner, ranks, reach, part, kv_heads, group)
        anywhere = pl.BlockSpec(memory_space=pl.ANY)
        dma = pltpu.SemaphoreType.DMA
        return pl.pallas_call(
            functools.partial(kernel, plan),
            out_shape=jax.ShapeDtypeStruct(queries.shape, jnp.bfloat16),
            in_specs=[pl.BlockSpec(memory_space=pltpu.SMEM), anywhere, anywhere, anywhere],
            out_specs=anywhere,
            scratch_shapes=[
                pltpu.VMEM((2, part, keys.shape[2]), jnp.bfloat16),
                pltpu.VMEM((part, queries.shape[2]), jnp.bfloat16),
                pltpu.VMEM((reach + 1, kv_heads, 2, 2, rows // 2, HD), jnp.bfloat16),
                pltpu.VMEM((kv_heads, rows, group * HD), jnp.bfloat16),
                pltpu.VMEM((kv_heads, rows, group * HD), jnp.bfloat16),
                pltpu.VMEM((rows, rows), jnp.float32),
                pltpu.VMEM((group, rows, rows), jnp.float32),
                pltpu.VMEM((1, rows), jnp.int32),
                pltpu.VMEM((kv_heads * group, 1, rows), jnp.float32),
                pltpu.VMEM((kv_heads * group, 1, rows), jnp.float32),
                pltpu.VMEM((kv_heads * group, HD, rows), jnp.float32),
                dma((3,)),
                dma((kv_heads, 3)),
                dma((heads, kv_heads, 2)),
                dma((heads, kv_heads, 2)),
                dma((heads, kv_heads)),
                dma((heads, kv_heads)),
                dma((reach + 1, kv_heads, 2)),
                dma((reach + 1, kv_heads, 2)),
                dma((2, kv_heads, 2)),
                dma((reach + 1, kv_heads, 2)),
                dma((heads, kv_heads)),
                dma((heads, kv_heads)),
                dma((kv_heads,)),
            ],
            compiler_params=pltpu.CompilerParams(
                collective_id=0, has_side_effects=True, vmem_limit_bytes=60 * 1024 * 1024
            ),
            name="attention",
        )(doc_lengths, queries, keys, values)

    split = P(("outer", "inner"), "head", None)
    return jax.shard_map(
        body, mesh=mesh, in_specs=(split, split, split, P()), out_specs=split, check_vma=False
    )
```
